32 devices in a mesh: mod: 4 (over y, x), seq: 8 (over z, core).
Axes of the slice: x: 2, y: 2, z: 4, core: 2. Of those that a mesh axis runs over, the one named last changes fastest.
Arguments:
- tokens: bfloat16 [2048, 4096], P(('mod', 'seq')), may hold values from -6 to 6
- norm_gain: float32 [3, 4096], replicated, may hold values from 0.2 to 2.6
- qkv_weight: bfloat16 [3, 4096, 12288], P(None, None, 'seq'), may hold values from -0.45 to 0.45
- out_weight: bfloat16 [3, 4096, 4096], P(None, 'seq'), may hold values from -0.375 to 0.375
- modality: int32 [16], replicated, may hold values from 0 to 2
- doc_lengths: int32 [4], replicated, may hold values from 1 to 1024, 2048 in all
Outputs:
- mixed: bfloat16 [2048, 4096], P(('mod', 'seq'))
The draws below stay inside these ranges and needn't reach their ends.
Inputs may be any that keep to these rules, and one draw needn't show every extreme that they name: `doc_lengths`: the lengths sum to 2048; documents follow one another from position 0 in the given order.
All inputs are finite; a program needn't handle non-finite values.
Results may differ from the reference program's by a relative error of at most 0.015.
Values may be sent and summed in bfloat16 or wider, within the bound.
A program may use at most 128 MiB of HBM per device.

```python
import math
import jax
import jax.numpy as jnp
import numpy as np
from jax import lax

D = 4096
HEADS = 32
HDIM = 128
MODS = 3
DOCS = 4
BLOCK = 128
TOKENS = 2048
BLOCKS = 16
HEAD_DEV = 4
FEATS = 4096
N_SEQ = 8


def draw_norm_gain(key, part):
    normal_draw = jax.random.uniform(jax.random.fold_in(key, 1), (MODS, D), jnp.float32, 0.6, 1.5)
    return normal_draw


def draw_qkv_weight(key, part):
    normal_draw = jax.random.normal(jax.random.fold_in(key, 3), (MODS, D, HEADS, 3, HDIM), jnp.float32)
    fan_scale = 1.0 / jnp.sqrt(jnp.float32(D))
    shared = normal_draw[:, :, :, 0:1, :] * 1.2 * fan_scale
    key_part = normal_draw[:, :, :, 1:2, :] * 1.2 * fan_scale
    values = normal_draw[:, :, :, 2:3, :] * fan_scale
    stacked = jnp.concatenate([shared, key_part, values], axis=3)
    return jnp.clip(stacked, -0.45, 0.45).reshape(MODS, D, HEADS * 3 * HDIM).astype(jnp.bfloat16)


def plant(values, rng, low, largest):
    spot = [jax.random.randint(jax.random.fold_in(rng, axis), (), 0, length) for axis, length in enumerate(values.shape)]
    widest = values.shape.index(max(values.shape))
    beside = spot[:widest] + [(spot[widest] + 1) % values.shape[widest]] + spot[widest + 1:]
    return values.at[tuple(spot)].set(low).at[tuple(beside)].set(largest)


def block_levels(key, dims, split, smallest, high):
    gain, own = 1.0, jax.random.fold_in(key, 6)
    for axis_at, blocks in split:
        draws = jnp.exp(jax.random.uniform(jax.random.fold_in(own, axis_at), (blocks,), jnp.float32, smallest / len(split), high / len(split)))
        gain = gain * jnp.repeat(draws, dims[axis_at] // blocks).reshape([-1 if axis == axis_at else 1 for axis in range(len(dims))])
    return gain


def rank_bounds(amount, slope):
    loads = [(1 << 20) // math.isqrt(grade ** slope) + 1 for grade in range(1, amount + 1)]
    spread = 1 + sum(loads) // (1 << 30)
    return np.cumsum(np.array([max(1, weight // spread) for weight in loads]))


def ranked(own_key, extent, amount, lean):
    grid = rank_bounds(amount, lean)
    lot = jax.random.randint(jax.random.fold_in(own_key, 1), extent, 0, int(grid[amount - 1]))
    grade = jnp.searchsorted(jnp.asarray(grid, jnp.int32), lot, side="right")
    return jax.random.permutation(jax.random.fold_in(own_key, 2), amount)[grade].astype(jnp.int32)


def profile(count, total, most, slope):
    weights = [(1 << 20) // math.isqrt(rank ** slope) + 1 for rank in range(2, count + 1)]
    surplus, counts = total - most - (count - 1), [1] * (count - 1)
    while surplus > 0:
        free = [i for i in range(count - 1) if counts[i] < most]
        whole, remaining = sum([weights[i] for i in free]), surplus
        for i in free:
            addition = min(most - counts[i], max(1, remaining * weights[i] // whole), surplus)
            counts[i] = counts[i] + addition
            surplus = surplus - addition
    return np.array([most] + counts)


def ragged_sizes(key, amount, total, limit, lean):
    if amount == 2:
        one = jax.random.randint(key, (), max(1, total - limit), min(limit, total - 1) + 1)
        return jnp.stack([one, total - one])
    sizes = jnp.asarray(profile(amount, total, limit, lean), jnp.int32)
    twos = (amount - 1) // 2
    donor, receiver = sizes[1:1 + 2 * twos:2], sizes[2:2 + 2 * twos:2]
    margin = jnp.minimum(donor - 1, limit - receiver)
    passed = jax.random.randint(jax.random.fold_in(key, 1), (twos,), 0, 1 << 20) % (margin + 1)
    sizes = sizes.at[1:1 + 2 * twos:2].set(donor - passed).at[2:2 + 2 * twos:2].set(receiver + passed)
    return sizes[jax.random.permutation(jax.random.fold_in(key, 2), amount)]


def scatter_about(rng, extent, deviation, limit, shards=(), kind=jnp.bfloat16):
    values = jax.random.normal(rng, extent, jnp.float32) * deviation
    if len(shards) > 0:
        values = block_levels(rng, extent, shards, -0.22, 0.18) * values
    return jnp.clip(values, min=-limit, max=limit).astype(kind)


def setup_inputs(seed: int = 0) -> dict:
    arg_keys = jax.random.split(jax.random.key(seed), 7)
    return {
        "tokens": scatter_about(arg_keys[0], (TOKENS, D), 1.0, 6.0, ((0, 32),)),
        "norm_gain": draw_norm_gain(jax.random.fold_in(arg_keys[6], 71), 0),
        "qkv_weight": draw_qkv_weight(jax.random.fold_in(arg_keys[6], 71), 0),
        "out_weight": scatter_about(arg_keys[3], (MODS, FEATS, D), (FEATS // 16) ** -0.5, 0.375, ((1, 8),)),
        "modality": plant(ranked(arg_keys[4], (BLOCKS,), MODS, 2), jax.random.fold_in(arg_keys[4], 3), 0, MODS - 1).astype(jnp.int32),
        "doc_lengths": ragged_sizes(arg_keys[5], DOCS, TOKENS, TOKENS // 2, 1).astype(jnp.int32),
    }


def reference(tokens, norm_gain, qkv_weight, out_weight, modality, doc_lengths):
    block_rows = tokens.reshape(BLOCKS, BLOCK, D).astype(jnp.float32)
    gain_rows = norm_gain[modality.astype(jnp.int32)]
    mean_square = lax.optimization_barrier(jnp.mean(block_rows * block_rows, axis=2, keepdims=True))
    normed = (block_rows * lax.rsqrt(mean_square + 1e-05) * gain_rows[:, None, :]).astype(jnp.bfloat16)

    def project(block_pair):
        row_block, block_mode = block_pair
        weight = lax.dynamic_index_in_dim(qkv_weight, block_mode, 0, keepdims=False)
        return jnp.dot(row_block, weight, preferred_element_type=jnp.float32).astype(jnp.bfloat16)
    projected = lax.map(project, (normed, modality))
    heads_first = jnp.moveaxis(projected.reshape(TOKENS, HEADS, 3, HDIM), 1, 0)
    doc_ends = jnp.cumsum(doc_lengths).astype(jnp.int32)
    position = jnp.arange(TOKENS, dtype=jnp.int32)
    document = lax.optimization_barrier(jnp.sum((position[:, None] >= doc_ends[None, :]).astype(jnp.int32), axis=1))
    allowed = (position[None, :] <= position[:, None]) & (document[None, :] == document[:, None])
    score_scale = 1.0 / math.sqrt(HDIM)

    def attend(one_head):
        scores = jnp.dot(one_head[:, 0, :], one_head[:, 1, :].T, preferred_element_type=jnp.float32) * score_scale
        row_max = lax.optimization_barrier(jnp.max(jnp.where(allowed, scores, -1e+30), axis=1, keepdims=True))
        weights = jnp.where(allowed, jnp.exp(scores - row_max), 0.0)
        totals = lax.optimization_barrier(jnp.sum(weights, axis=1, keepdims=True))
        summed = jnp.dot(weights.astype(jnp.bfloat16), one_head[:, 2, :], preferred_element_type=jnp.float32)
        return (summed / totals).astype(jnp.bfloat16)
    attended = lax.map(attend, heads_first)
    merged = jnp.moveaxis(attended, 0, 1).reshape(BLOCKS, BLOCK, N_SEQ, HEAD_DEV * HDIM)

    def output(block_pair):
        row_block, block_mode = block_pair
        weight = lax.dynamic_index_in_dim(out_weight, block_mode, 0, keepdims=False)
        weight = weight.reshape(N_SEQ, HEAD_DEV * HDIM, D).astype(jnp.float32)
        parts = jnp.einsum('bgc,gcd->gbd', row_block.astype(jnp.float32), weight)
        rounded = lax.optimization_barrier(parts.astype(jnp.bfloat16))
        return lax.optimization_barrier(jnp.sum(rounded.astype(jnp.float32), axis=0))
    projected_back = lax.map(output, (merged, modality)).reshape(TOKENS, D)
    return (tokens.astype(jnp.float32) + projected_back).astype(jnp.bfloat16)
```

```python
import functools
import math

import jax
import jax.numpy as jnp
from jax import lax
from jax.experimental import pallas as pl
from jax.experimental.pallas import tpu as pltpu
from jax.sharding import PartitionSpec as P

HDIM = 128
MESH = pl.DeviceIdType.MESH
F32 = jnp.float32
BF16 = jnp.bfloat16


def mul(x, k):
    return pl.multiple_of(x, k)


def remote(src, dst, send, recv, dev):
    return pltpu.make_async_remote_copy(
        src_ref=src, dst_ref=dst, send_sem=send, recv_sem=recv,
        device_id=dev, device_id_type=MESH,
    )


def greet(devs):
    barrier = pltpu.get_barrier_semaphore()
    for dev in devs:
        pl.semaphore_signal(barrier, inc=1, device_id=dev, device_id_type=MESH)
    pl.semaphore_wait(barrier, len(devs))


def gather_project(
    n, modality, tokens, gain, w_hbm, q_out, kv_out, wv, xg, stage,
    w_sem, rs, rr, ls, lr, ps, pr, a_s, a_r, b_s, b_r,
):
    m = lax.axis_index("mod")
    s = lax.axis_index("seq")
    chip, core = s // 2, s % 2
    rows, width = tokens.shape
    pair = 2 * rows
    group = n * pair
    half = n // 2
    feats = q_out.shape[1]
    heads = feats // HDIM
    mods = w_hbm.shape[0]
    right = (m, ((chip + 1) % n) * 2 + core)
    left = (m, ((chip + n - 1) % n) * 2 + core)
    partner = (m, chip * 2 + (1 - core))

    w_copies = [pltpu.make_async_copy(w_hbm.at[k], wv.at[k], w_sem.at[k]) for k in range(mods)]
    for c in w_copies:
        c.start()

    def block_rows(offset):
        return mul(((chip + offset + n) % n) * pair, pair)

    def at(offset, which, first=0, count=rows):
        return xg.at[pl.ds(mul(block_rows(offset) + which * rows + first, count), count), :]

    values = tokens[...].astype(F32)
    inv = lax.rsqrt(jnp.mean(values * values, axis=1, keepdims=True) + 1e-05)
    row_gain = gain[pl.ds(modality[m * n + chip], 1), :]
    xg[pl.ds(mul(block_rows(0) + core * rows, rows), rows), :] = (values * inv * row_gain).astype(BF16)

    @pl.when(m < 2)
    def _():
        kv_out[pl.ds(0, group), :] = jnp.zeros((group, 2 * feats), BF16)

    @pl.when(m < 1)
    def _():
        kv_out[pl.ds(group, group), :] = jnp.zeros((group, 2 * feats), BF16)

    others = [((m + d) % 4, s) for d in range(1, 4)]
    greet([right, left, partner] + others)

    def going(k, part, to, ssem, rsem, sign):
        off = -sign * (k - 1)
        if part is None:
            ref = at(off, core)
        else:
            ref = at(off, core, part * (rows // 2), rows // 2)
        return remote(ref, ref, ssem.at[k - 1], rsem.at[k - 1], to)

    def right_copy(k):
        return going(k, 0 if k == half else None, right, rs, rr, 1)

    def left_copy(k):
        return going(k, 1 if k == half else None, left, ls, lr, -1)

    def landed(k, sign, rsem, ssem):
        off = -sign * k
        if k == half:
            ref = at(off, core, (0 if sign > 0 else rows // 2), rows // 2)
        else:
            ref = at(off, core)
        return remote(ref, ref, ssem.at[k - 1], rsem.at[k - 1], right)

    def partner_copy(off, which):
        ref = at(off, core)
        return remote(ref, ref, ps.at[which], pr.at[which], partner)

    def partner_landed(off, which):
        ref = at(off, 1 - core)
        return remote(ref, ref, ps.at[which], pr.at[which], partner)

    sent = []

    def go(copy):
        copy.start()
        sent.append(copy)

    go(right_copy(1))
    go(left_copy(1))
    go(partner_copy(0, 0))

    tile = 256 if (3 * feats) % 256 == 0 else 128

    def own_copies(t, r):
        src = kv_out.at[pl.ds(mul(2 * group + r, pair), pair), :]
        near = kv_out.at[pl.ds(mul(group + r, pair), pair), :]
        far = kv_out.at[pl.ds(r, pair), :]
        return {
            0: [remote(src, near, a_s.at[t], a_r.at[t], (1, s)), remote(src, far, b_s.at[t], b_r.at[t], (2, s))],
            1: [remote(src, far, b_s.at[t], b_r.at[t], (3, s))],
            2: [remote(src, near, a_s.at[t], a_r.at[t], (3, s))],
            3: [remote(far, near, a_s.at[t], a_r.at[t], (2, s))],
        }

    plan = []

    def project(off):
        t = len(plan)
        r = block_rows(off)
        mode = modality[m * n + (chip + off + n) % n]

        def one_tile(j, carry):
            cols = pl.ds(mul(j * tile, tile), tile)
            stage[:, cols] = jnp.dot(
                xg[pl.ds(r, pair), :], wv[mode, :, cols], preferred_element_type=F32
            ).astype(BF16)
            return carry

        lax.fori_loop(0, 3 * feats // tile, one_tile, 0)
        for h in range(heads):
            q_out[pl.ds(r, pair), pl.ds(h * HDIM, HDIM)] = stage[:, pl.ds(3 * h * HDIM, HDIM)]
            kv_out[pl.ds(mul(2 * group + r, pair), pair), pl.ds(2 * h * HDIM, 2 * HDIM)] = stage[
                :, pl.ds((3 * h + 1) * HDIM, 2 * HDIM)
            ]
        copies = own_copies(t, r)
        plan.append(copies)
        for who in range(3):
            @pl.when(m == who)
            def _(who=who):
                for c in copies[who]:
                    c.start()
        forward_to(t)

    forwarded = []

    def forward_to(count):
        for t in range(len(forwarded), count):
            forwarded.append(t)

            @pl.when(m == 3)
            def _(t=t):
                plan[t][1][0].wait_recv()
                plan[t][3][0].start()

    for c in w_copies:
        c.wait()
    next_pair = 1
    for k in range(1, half):
        landed(k, 1, rr, rs).wait_recv()
        go(right_copy(k + 1))
        landed(k, -1, lr, ls).wait_recv()
        go(left_copy(k + 1))
        go(partner_copy(-k, next_pair))
        go(partner_copy(k, next_pair + 1))
        if k == 1:
            partner_landed(0, 0).wait_recv()
            project(0)
        partner_landed(-k, next_pair).wait_recv()
        project(-k)
        if k == half - 1:
            landed(half, 1, rr, rs).wait_recv()
            landed(half, -1, lr, ls).wait_recv()
            go(partner_copy(half, next_pair + 2))
        partner_landed(k, next_pair + 1).wait_recv()
        project(k)
        next_pair += 2
    partner_landed(half, next_pair).wait_recv()
    project(half)
    forward_to(n)
    for copy in sent:
        copy.wait_send()
    for who in range(4):
        @pl.when(m == who)
        def _(who=who):
            for copies in plan:
                for c in copies[who]:
                    c.wait_send()
                if who in (1, 3):
                    copies[0 if who == 1 else 2][0].wait_recv()
                if who == 2:
                    copies[3][0].wait_recv()
                    copies[0][1].wait_recv()


def attend_reduce(
    n, modality, doc_lengths, tokens, q, kv, w_hbm, out, wv, att, part, pairbuf, bias, right_in, left_in,
    w_sem, ps, pr, rs, rr, ls, lr,
):
    m = lax.axis_index("mod")
    s = lax.axis_index("seq")
    chip, core = s // 2, s % 2
    rows, width = tokens.shape
    pair = 2 * rows
    group = n * pair
    half = n // 2
    feats = q.shape[1]
    heads = feats // HDIM
    mods = w_hbm.shape[0]
    right = (m, ((chip + 1) % n) * 2 + core)
    left = (m, ((chip + n - 1) % n) * 2 + core)
    partner = (m, chip * 2 + (1 - core))
    w_copies = [pltpu.make_async_copy(w_hbm.at[k], wv.at[k], w_sem.at[k]) for k in range(mods)]
    for c in w_copies:
        c.start()
    greet([right, left, partner])

    keys = 3 * group
    chunk = keys
    while chunk > 1536:
        chunk //= 2
    scale = math.log2(math.e) / math.sqrt(HDIM)
    first_key = (m - 2) * group
    mine = pl.ds(mul(core * rows, rows), rows)
    theirs = pl.ds(mul((1 - core) * rows, rows), rows)
    waited = []

    def compute(t, off):
        r = mul(((chip + off + n) % n) * pair, pair)
        pos = m * group + r + lax.broadcasted_iota(jnp.int32, (pair, 1), 0)
        end = jnp.int32(0)
        start = jnp.zeros((pair, 1), jnp.int32)
        for d in range(doc_lengths.shape[0]):
            end = end + doc_lengths[d]
            start = jnp.where(pos >= end, end, start)
        for c0 in range(0, keys, chunk):
            key = first_key + c0 + lax.broadcasted_iota(jnp.int32, (pair, chunk), 1)
            bias[:, pl.ds(c0, chunk)] = jnp.where((key <= pos) & (key >= start), 0.0, -1e30)
        for h in range(heads):
            query = q[pl.ds(r, pair), pl.ds(h * HDIM, HDIM)]
            top = total = acc = None
            for c0 in reversed(range(0, keys, chunk)):
                k_part = kv[pl.ds(c0, chunk), pl.ds(2 * h * HDIM, HDIM)]
                v_part = kv[pl.ds(c0, chunk), pl.ds((2 * h + 1) * HDIM, HDIM)]
                scores = lax.dot_general(
                    query, k_part, (((1,), (1,)), ((), ())), preferred_element_type=F32
                ) * scale + bias[:, pl.ds(c0, chunk)]
                peak = jnp.max(scores, axis=1, keepdims=True)
                new_top = peak if top is None else jnp.maximum(top, peak)
                weights = jnp.exp2(scores - new_top)
                if chunk != keys:
                    weights = jnp.where(bias[:, pl.ds(c0, chunk)] < 0.0, 0.0, weights)
                row_sum = jnp.sum(weights, axis=1, keepdims=True)
                added = jnp.dot(weights.astype(BF16), v_part, preferred_element_type=F32)
                if top is None:
                    total, acc = row_sum, added
                else:
                    fix = jnp.exp2(top - new_top)
                    total, acc = total * fix + row_sum, acc * fix + added
                top = new_top
            att[:, pl.ds(h * HDIM, HDIM)] = (acc / total).astype(BF16)
        if not waited:
            for c in w_copies:
                c.wait()
            waited.append(True)
        mode = modality[m * n + (chip + off + n) % n]
        tile = 512

        def one_tile(j, carry):
            cols = pl.ds(mul(j * tile, tile), tile)
            part[t, :, cols] = jnp.dot(
                att[...], wv[mode, :, cols], preferred_element_type=F32
            ).astype(BF16)
            return carry

        lax.fori_loop(0, width // tile, one_tile, 0)
        copy = remote(part.at[t, theirs, :], pairbuf.at[t], ps.at[t], pr.at[t], partner)
        copy.start()
        return copy

    lo, hi = pl.ds(0, width // 2), pl.ds(width // 2, width // 2)
    sent = []

    def pair_sum(t, copy):
        copy.wait_recv()
        sent.append(copy)
        return part[t, mine, :].astype(F32) + pairbuf[t].astype(F32)

    def send(src, dst, ss, rsm, dev):
        copy = remote(src, dst, ss, rsm, dev)
        copy.start()
        sent.append(copy)
        return copy

    copy = compute(0, half)
    part[0, mine, :] = pair_sum(0, copy).astype(BF16)
    r_prev = send(part.at[0, mine, lo], right_in.at[half - 1, :, lo], rs.at[half - 1], rr.at[half - 1], right)
    l_prev = send(part.at[0, mine, hi], left_in.at[half - 1, :, hi], ls.at[half - 1], lr.at[half - 1], left)
    t = 1
    for k in range(half - 1, 0, -1):
        c_right = compute(t, k)
        c_left = compute(t + 1, -k)
        for which, (tt, c, prev, inbox, ss, rsm, dev, cols) in enumerate((
            (t, c_right, r_prev, right_in, rs, rr, right, lo),
            (t + 1, c_left, l_prev, left_in, ls, lr, left, hi),
        )):
            total = pair_sum(tt, c)
            prev.wait_recv()
            if k == half - 1:
                a, b = total[:, : width // 2], total[:, width // 2:]
                if which == 0:
                    a = a + inbox[k, :, lo].astype(F32)
                else:
                    b = b + inbox[k, :, hi].astype(F32)
                part[tt, mine, lo] = a.astype(BF16)
                part[tt, mine, hi] = b.astype(BF16)
            else:
                part[tt, mine, :] = (total + inbox[k].astype(F32)).astype(BF16)
            new = send(part.at[tt, mine, :], inbox.at[k - 1], ss.at[k - 1], rsm.at[k - 1], dev)
            if which == 0:
                r_prev = new
            else:
                l_prev = new
        t += 2
    c = compute(t, 0)
    total = pair_sum(t, c) + tokens[...].astype(F32)
    r_prev.wait_recv()
    total = total + right_in[0].astype(F32)
    l_prev.wait_recv()
    out[...] = (total + left_in[0].astype(F32)).astype(BF16)
    for copy in sent:
        copy.wait_send()


def body(n, tokens, norm_gain, qkv_weight, out_weight, modality, doc_lengths):
    rows, width = tokens.shape
    feats = out_weight.shape[1]
    mods = out_weight.shape[0]
    pair = 2 * rows
    group = n * pair
    half = n // 2
    vmem = pl.BlockSpec(memory_space=pltpu.VMEM)
    smem = pl.BlockSpec(memory_space=pltpu.SMEM)
    hbm = pl.BlockSpec(memory_space=pl.ANY)
    dma = pltpu.SemaphoreType.DMA
    limit = 62 * 1024 * 1024
    q, kv = pl.pallas_call(
        functools.partial(gather_project, n),
        out_shape=(
            jax.ShapeDtypeStruct((group, feats), BF16),
            jax.ShapeDtypeStruct((3 * group, 2 * feats), BF16),
        ),
        in_specs=[smem, vmem, vmem, hbm],
        out_specs=(vmem, vmem),
        scratch_shapes=[
            pltpu.VMEM((mods, width, 3 * feats), BF16),
            pltpu.VMEM((group, width), BF16),
            pltpu.VMEM((pair, 3 * feats), BF16),
            dma((mods,)),
            dma((half,)), dma((half,)), dma((half,)), dma((half,)),
            dma((n,)), dma((n,)),
            dma((n,)), dma((n,)), dma((n,)), dma((n,)),
        ],
        compiler_params=pltpu.CompilerParams(
            collective_id=0, has_side_effects=True, vmem_limit_bytes=limit
        ),
    )(modality, tokens, norm_gain, qkv_weight)
    return pl.pallas_call(
        functools.partial(attend_reduce, n),
        out_shape=jax.ShapeDtypeStruct((rows, width), BF16),
        in_specs=[smem, smem, vmem, vmem, vmem, hbm],
        out_specs=vmem,
        scratch_shapes=[
            pltpu.VMEM((mods, feats, width), BF16),
            pltpu.VMEM((pair, feats), BF16),
            pltpu.VMEM((n, pair, width), BF16),
            pltpu.VMEM((n, rows, width), BF16),
            pltpu.VMEM((pair, 3 * group), F32),
            pltpu.VMEM((half, rows, width), BF16),
            pltpu.VMEM((half, rows, width), BF16),
            dma((mods,)),
            dma((n,)), dma((n,)),
            dma((half,)), dma((half,)), dma((half,)), dma((half,)),
        ],
        compiler_params=pltpu.CompilerParams(
            collective_id=1, has_side_effects=True, vmem_limit_bytes=limit
        ),
    )(modality, doc_lengths, tokens, q, kv, out_weight)


def solution(mesh):
    return jax.shard_map(
        functools.partial(body, mesh.shape["seq"] // 2),
        mesh=mesh,
        in_specs=(
            P(("mod", "seq"), None),
            P(),
            P(None, None, "seq"),
            P(None, "seq", None),
            P(),
            P(),
        ),
        out_specs=P(("mod", "seq"), None),
        check_vma=False,
    )
```

```python
import functools
import math

import jax
import jax.numpy as jnp
from jax import lax
from jax.experimental import pallas as pl
from jax.experimental.pallas import tpu as pltpu
from jax.sharding import PartitionSpec as P

HDIM = 128
MESH = pl.DeviceIdType.MESH
F32 = jnp.float32
BF16 = jnp.bfloat16


def mul(x, k):
    return pl.multiple_of(x, k)


def remote(src, dst, send, recv, dev):
    return pltpu.make_async_remote_copy(
        src_ref=src, dst_ref=dst, send_sem=send, recv_sem=recv,
        device_id=dev, device_id_type=MESH,
    )


def greet(devs):
    barrier = pltpu.get_barrier_semaphore()
    for dev in devs:
        pl.semaphore_signal(barrier, inc=1, device_id=dev, device_id_type=MESH)
    pl.semaphore_wait(barrier, len(devs))


def sublayer(
    n, modality, doc_lengths, tokens, gain, w_hbm, o_hbm, out,
    wv, xg, stage, q_out, kv_out, att, pairbuf, bias, right_in, left_in,
    w_sem, o_sem, own_s, fs, fr, ps, pr, a_s, a_r, b_s, b_r, ps2, pr2, rs, rr, ls, lr,
):
    m = lax.axis_index("mod")
    s = lax.axis_index("seq")
    chip, core = s // 2, s % 2
    rows, width = tokens.shape
    pair = 2 * rows
    group = n * pair
    half = n // 2
    feats = q_out.shape[1]
    heads = feats // HDIM
    mods = w_hbm.shape[0]
    right = (m, ((chip + 1) % n) * 2 + core)
    left = (m, ((chip + n - 1) % n) * 2 + core)
    partner = (m, chip * 2 + (1 - core))
    chunks = 2
    piece = rows // chunks

    w_copies = [pltpu.make_async_copy(w_hbm.at[k], wv.at[k], w_sem.at[k]) for k in range(mods)]
    for c in w_copies:
        c.start()

    values = tokens[...].astype(F32)
    inv = lax.rsqrt(jnp.mean(values * values, axis=1, keepdims=True) + 1e-05)
    row_gain = gain[pl.ds(modality[m * n + chip], 1), :]
    xg[pl.ds(mul(chip * pair + core * rows, rows), rows), :] = (values * inv * row_gain).astype(BF16)

    @pl.when(m < 2)
    def _():
        kv_out[pl.ds(0, group), :] = jnp.zeros((group, 2 * feats), BF16)

    @pl.when(m < 1)
    def _():
        kv_out[pl.ds(group, group), :] = jnp.zeros((group, 2 * feats), BF16)

    others = [((m + d) % 4, s) for d in range(1, 4)]
    greet([right, left, partner] + others)

    def ref(block, which, c):
        return xg.at[pl.ds(mul(block * pair + which * rows + c * piece, piece), piece), :]

    def to_partner(block, c):
        r = ref(block, core, c)
        return remote(r, r, ps.at[block, c], pr.at[block, c], partner)

    def from_partner(block, c):
        r = ref(block, 1 - core, c)
        return remote(r, r, ps.at[block, c], pr.at[block, c], partner)

    def onward(block, c, dev, sem):
        r = ref(block, core, c)
        return remote(r, r, sem, fr.at[block, c], dev)

    for c in range(chunks):
        @pl.when(chip < n - 1)
        def _(c=c):
            onward(chip, c, right, own_s.at[0, c]).start()

        @pl.when(chip > 0)
        def _(c=c):
            onward(chip, c, left, own_s.at[1, c]).start()
    for c in range(chunks):
        to_partner(chip, c).start()

    def handle(k, c):
        for sign, dev in ((-1, right), (1, left)):
            block = chip + sign * k
            following = chip - sign

            @pl.when((block >= 0) & (block < n))
            def _(block=block, following=following, dev=dev):
                onward(block, c, dev, fs.at[block, c]).wait_recv()

                @pl.when((following >= 0) & (following < n))
                def _():
                    onward(block, c, dev, fs.at[block, c]).start()

                to_partner(block, c).start()

    def settle():
        for c in range(chunks):
            @pl.when(chip < n - 1)
            def _(c=c):
                onward(chip, c, right, own_s.at[0, c]).wait_send()

            @pl.when(chip > 0)
            def _(c=c):
                onward(chip, c, left, own_s.at[1, c]).wait_send()

            for d in range(n):
                to_partner((chip + d) % n, c).wait_send()
            for k in range(1, n):
                for sign, dev in ((-1, right), (1, left)):
                    block = chip + sign * k
                    following = chip - sign

                    @pl.when((block >= 0) & (block < n) & (following >= 0) & (following < n))
                    def _(block=block, dev=dev, c=c):
                        onward(block, c, dev, fs.at[block, c]).wait_send()

    tile = 256 if (3 * feats) % 256 == 0 else 128
    upper = chip // half
    near_side = chip * (1 - upper) + (n - 1 - chip) * upper
    far_sign = 1 - 2 * upper

    def block_at(t):
        if t == 0:
            return chip
        step = (t + 1) // 2
        two = step if t % 2 == 0 else -step
        past = (t - 1 - 2 * near_side + 2 * n) // (2 * n)
        return chip + two * (1 - past) + far_sign * (t - near_side) * past

    def own_copies(t, r):
        src = kv_out.at[pl.ds(mul(2 * group + r, pair), pair), :]
        near = kv_out.at[pl.ds(mul(group + r, pair), pair), :]
        far = kv_out.at[pl.ds(r, pair), :]
        return {
            0: [remote(src, near, a_s.at[t], a_r.at[t], (1, s)), remote(src, far, b_s.at[t], b_r.at[t], (2, s))],
            1: [remote(src, far, b_s.at[t], b_r.at[t], (3, s))],
            2: [remote(src, near, a_s.at[t], a_r.at[t], (3, s))],
            3: [remote(far, near, a_s.at[t], a_r.at[t], (2, s))],
        }

    plan = []
    forwarded = []

    def forward_to(count):
        for t in range(len(forwarded), count):
            forwarded.append(t)

            @pl.when(m == 3)
            def _(t=t):
                plan[t][1][0].wait_recv()
                plan[t][3][0].start()

    def project():
        t = len(plan)
        block = block_at(t)
        r = mul(block * pair, pair)
        mode = modality[m * n + block]
        for c in range(chunks):
            from_partner(block, c).wait_recv()

        def one_tile(j, carry):
            cols = pl.ds(mul(j * tile, tile), tile)
            stage[:, cols] = jnp.dot(
                xg[pl.ds(r, pair), :], wv[mode, :, cols], preferred_element_type=F32
            ).astype(BF16)
            return carry

        lax.fori_loop(0, 3 * feats // tile, one_tile, 0)
        for h in range(heads):
            q_out[pl.ds(r, pair), pl.ds(h * HDIM, HDIM)] = stage[:, pl.ds(3 * h * HDIM, HDIM)]
            kv_out[pl.ds(mul(2 * group + r, pair), pair), pl.ds(2 * h * HDIM, 2 * HDIM)] = stage[
                :, pl.ds((3 * h + 1) * HDIM, 2 * HDIM)
            ]
        copies = own_copies(t, r)
        plan.append(copies)
        for who in range(3):
            @pl.when(m == who)
            def _(who=who):
                for c in copies[who]:
                    c.start()
        forward_to(t)

    for c in range(chunks - 1):
        handle(1, c)
    for c in w_copies:
        c.wait()
    project()
    handle(1, chunks - 1)
    project()
    for k in range(2, n):
        for c in range(chunks):
            handle(k, c)
        project()
    squares = width // feats
    o_copies = [
        pltpu.make_async_copy(
            o_hbm.at[k, :, pl.ds(c * feats, feats)],
            wv.at[k, pl.ds(c * feats, feats), pl.ds(0, feats)],
            o_sem.at[k * squares + c],
        )
        for c in range(squares) for k in range(mods)
    ]
    for c in o_copies:
        c.start()
    forward_to(n)
    settle()
    for who in range(4):
        @pl.when(m == who)
        def _(who=who):
            for copies in plan:
                if who in (1, 3):
                    copies[0 if who == 1 else 2][0].wait_recv()
                if who == 2:
                    copies[3][0].wait_recv()
                    copies[0][1].wait_recv()

    q, kv = q_out, kv_out
    keys = 3 * group
    chunk = keys
    while chunk > 1536:
        chunk //= 2
    scale = math.log2(math.e) / math.sqrt(HDIM)
    first_key = (m - 2) * group
    def mine(t):
        return pl.ds(mul(t * pair + core * rows, rows), rows)

    def theirs(t):
        return pl.ds(mul(t * pair + (1 - core) * rows, rows), rows)

    waited = []

    def compute(t, off):
        r = mul(((chip + off + n) % n) * pair, pair)
        pos = m * group + r + lax.broadcasted_iota(jnp.int32, (pair, 1), 0)
        end = jnp.int32(0)
        start = jnp.zeros((pair, 1), jnp.int32)
        for d in range(doc_lengths.shape[0]):
            end = end + doc_lengths[d]
            start = jnp.where(pos >= end, end, start)
        for c0 in range(0, keys, chunk):
            key = first_key + c0 + lax.broadcasted_iota(jnp.int32, (pair, chunk), 1)
            bias[:, pl.ds(c0, chunk)] = jnp.where((key <= pos) & (key >= start), 0.0, -1e30)
        for h in range(heads):
            query = q[pl.ds(r, pair), pl.ds(h * HDIM, HDIM)]
            top = total = acc = None
            for c0 in reversed(range(0, keys, chunk)):
                k_part = kv[pl.ds(c0, chunk), pl.ds(2 * h * HDIM, HDIM)]
                v_part = kv[pl.ds(c0, chunk), pl.ds((2 * h + 1) * HDIM, HDIM)]
                scores = lax.dot_general(
                    query, k_part, (((1,), (1,)), ((), ())), preferred_element_type=F32
                ) * scale + bias[:, pl.ds(c0, chunk)]
                peak = jnp.max(scores, axis=1, keepdims=True)
                new_top = peak if top is None else jnp.maximum(top, peak)
                weights = jnp.exp2(scores - new_top)
                if chunk != keys:
                    weights = jnp.where(bias[:, pl.ds(c0, chunk)] < 0.0, 0.0, weights)
                row_sum = jnp.sum(weights, axis=1, keepdims=True)
                added = jnp.dot(weights.astype(BF16), v_part, preferred_element_type=F32)
                if top is None:
                    total, acc = row_sum, added
                else:
                    fix = jnp.exp2(top - new_top)
                    total, acc = total * fix + row_sum, acc * fix + added
                top = new_top
            att[:, pl.ds(h * HDIM, HDIM)] = (acc / total).astype(BF16)
        if not waited:
            for c in o_copies:
                c.wait()
            waited.append(True)
        mode = modality[m * n + (chip + off + n) % n]

        def one_tile(j, carry):
            cols = pl.ds(mul(j * feats, feats), feats)
            square = wv[mode, cols, pl.ds(0, feats)]
            xg[pl.ds(t * pair, pair), cols] = jnp.dot(
                att[...], square, preferred_element_type=F32
            ).astype(BF16)
            return carry

        lax.fori_loop(0, squares, one_tile, 0)
        copy = remote(xg.at[theirs(t), :], pairbuf.at[t], ps2.at[t], pr2.at[t], partner)
        copy.start()
        return copy

    lo, hi = pl.ds(0, width // 2), pl.ds(width // 2, width // 2)
    sent = []

    def pair_sum(t, copy):
        copy.wait_recv()
        sent.append(copy)
        return xg[mine(t), :].astype(F32) + pairbuf[t].astype(F32)

    def send(src, dst, ss, rsm, dev):
        copy = remote(src, dst, ss, rsm, dev)
        copy.start()
        sent.append(copy)
        return copy

    copy = compute(0, half)
    xg[mine(0), :] = pair_sum(0, copy).astype(BF16)
    r_prev = send(xg.at[mine(0), lo], right_in.at[half - 1, :, lo], rs.at[half - 1], rr.at[half - 1], right)
    l_prev = send(xg.at[mine(0), hi], left_in.at[half - 1, :, hi], ls.at[half - 1], lr.at[half - 1], left)
    t = 1
    for k in range(half - 1, 0, -1):
        c_right = compute(t, k)
        c_left = compute(t + 1, -k)
        for which, (tt, c, prev, inbox, ss, rsm, dev, cols) in enumerate((
            (t, c_right, r_prev, right_in, rs, rr, right, lo),
            (t + 1, c_left, l_prev, left_in, ls, lr, left, hi),
        )):
            total = pair_sum(tt, c)
            prev.wait_recv()
            if k == half - 1:
                a, b = total[:, : width // 2], total[:, width // 2:]
                if which == 0:
                    a = a + inbox[k, :, lo].astype(F32)
                else:
                    b = b + inbox[k, :, hi].astype(F32)
                xg[mine(tt), lo] = a.astype(BF16)
                xg[mine(tt), hi] = b.astype(BF16)
            else:
                xg[mine(tt), :] = (total + inbox[k].astype(F32)).astype(BF16)
            new = send(xg.at[mine(tt), :], inbox.at[k - 1], ss.at[k - 1], rsm.at[k - 1], dev)
            if which == 0:
                r_prev = new
            else:
                l_prev = new
        t += 2
    c = compute(t, 0)
    total = pair_sum(t, c) + tokens[...].astype(F32)
    r_prev.wait_recv()
    total = total + right_in[0].astype(F32)
    l_prev.wait_recv()
    out[...] = (total + left_in[0].astype(F32)).astype(BF16)
    for copy in sent:
        copy.wait_send()


    for who in range(4):
        @pl.when(m == who)
        def _(who=who):
            for copies in plan:
                for c in copies[who]:
                    c.wait_send()


def body(n, tokens, norm_gain, qkv_weight, out_weight, modality, doc_lengths):
    rows, width = tokens.shape
    feats = out_weight.shape[1]
    mods = out_weight.shape[0]
    pair = 2 * rows
    group = n * pair
    half = n // 2
    vmem = pl.BlockSpec(memory_space=pltpu.VMEM)
    smem = pl.BlockSpec(memory_space=pltpu.SMEM)
    hbm = pl.BlockSpec(memory_space=pl.ANY)
    dma = pltpu.SemaphoreType.DMA
    limit = 62 * 1024 * 1024
    return pl.pallas_call(
        functools.partial(sublayer, n),
        out_shape=jax.ShapeDtypeStruct((rows, width), BF16),
        in_specs=[smem, smem, vmem, vmem, hbm, hbm],
        out_specs=vmem,
        scratch_shapes=[
            pltpu.VMEM((mods, width, 3 * feats), BF16),
            pltpu.VMEM((group, width), BF16),
            pltpu.VMEM((pair, 3 * feats), BF16),
            pltpu.VMEM((group, feats), BF16),
            pltpu.VMEM((3 * group, 2 * feats), BF16),
            pltpu.VMEM((pair, feats), BF16),
            pltpu.VMEM((n, rows, width), BF16),
            pltpu.VMEM((pair, 3 * group), F32),
            pltpu.VMEM((half, rows, width), BF16),
            pltpu.VMEM((half, rows, width), BF16),
            dma((mods,)), dma((mods * (width // feats),)),
            dma((2, 2)), dma((n, 2)), dma((n, 2)), dma((n, 2)), dma((n, 2)),
            dma((n,)), dma((n,)), dma((n,)), dma((n,)),
            dma((n,)), dma((n,)),
            dma((half,)), dma((half,)), dma((half,)), dma((half,)),
        ],
        compiler_params=pltpu.CompilerParams(
            collective_id=0, has_side_effects=True, vmem_limit_bytes=limit
        ),
    )(modality, doc_lengths, tokens, norm_gain, qkv_weight, out_weight)


def solution(mesh):
    return jax.shard_map(
        functools.partial(body, mesh.shape["seq"] // 2),
        mesh=mesh,
        in_specs=(
            P(("mod", "seq"), None),
            P(),
            P(None, None, "seq"),
            P(None, "seq", None),
            P(),
            P(),
        ),
        out_specs=P(("mod", "seq"), None),
        check_vma=False,
    )
```

```python
import functools
import math

import jax
import jax.numpy as jnp
from jax import lax
from jax.experimental import pallas as pl
from jax.experimental.pallas import tpu as pltpu
from jax.sharding import PartitionSpec as P

HDIM = 128
MESH = pl.DeviceIdType.MESH
F32 = jnp.float32
BF16 = jnp.bfloat16


def mul(x, k):
    return pl.multiple_of(x, k)


def remote(src, dst, send, recv, dev):
    return pltpu.make_async_remote_copy(
        src_ref=src, dst_ref=dst, send_sem=send, recv_sem=recv,
        device_id=dev, device_id_type=MESH,
    )


def greet(devs):
    barrier = pltpu.get_barrier_semaphore()
    for dev in devs:
        pl.semaphore_signal(barrier, inc=1, device_id=dev, device_id_type=MESH)
    pl.semaphore_wait(barrier, len(devs))


def sublayer(
    n, modality, doc_lengths, tokens, gain, w_hbm, o_hbm, out,
    wv, xg, stage, q_out, kv_out, att, pairbuf, bias, right_in, left_in,
    w_sem, o_sem, own_s, fs, fr, ps, pr, a_s, a_r, b_s, b_r, ps2, pr2, rs, rr, ls, lr,
):
    m = lax.axis_index("mod")
    s = lax.axis_index("seq")
    chip, core = s // 2, s % 2
    rows, width = tokens.shape
    pair = 2 * rows
    group = n * pair
    half = n // 2
    feats = q_out.shape[1]
    heads = feats // HDIM
    mods = w_hbm.shape[0]
    right = (m, ((chip + 1) % n) * 2 + core)
    left = (m, ((chip + n - 1) % n) * 2 + core)
    partner = (m, chip * 2 + (1 - core))
    chunks = 2
    piece = rows // chunks

    w_copies = [pltpu.make_async_copy(w_hbm.at[k], wv.at[k], w_sem.at[k]) for k in range(mods)]
    for c in w_copies:
        c.start()

    values = tokens[...].astype(F32)
    inv = lax.rsqrt(jnp.mean(values * values, axis=1, keepdims=True) + 1e-05)
    row_gain = gain[pl.ds(modality[m * n + chip], 1), :]
    xg[pl.ds(mul(chip * pair + core * rows, rows), rows), :] = (values * inv * row_gain).astype(BF16)

    @pl.when(m < 2)
    def _():
        kv_out[pl.ds(0, group), :] = jnp.zeros((group, 2 * feats), BF16)

    @pl.when(m < 1)
    def _():
        kv_out[pl.ds(group, group), :] = jnp.zeros((group, 2 * feats), BF16)

    others = [((m + d) % 4, s) for d in range(1, 4)]
    greet([right, left, partner] + others)

    def ref(block, which, c):
        return xg.at[pl.ds(mul(block * pair + which * rows + c * piece, piece), piece), :]

    def to_partner(block, c):
        r = ref(block, core, c)
        return remote(r, r, ps.at[block, c], pr.at[block, c], partner)

    def from_partner(block, c):
        r = ref(block, 1 - core, c)
        return remote(r, r, ps.at[block, c], pr.at[block, c], partner)

    def onward(block, c, dev, sem):
        r = ref(block, core, c)
        return remote(r, r, sem, fr.at[block, c], dev)

    for c in range(chunks):
        @pl.when(chip < n - 1)
        def _(c=c):
            onward(chip, c, right, own_s.at[0, c]).start()

        @pl.when(chip > 0)
        def _(c=c):
            onward(chip, c, left, own_s.at[1, c]).start()
    for c in range(chunks):
        to_partner(chip, c).start()

    def handle(k, c):
        for sign, dev in ((-1, right), (1, left)):
            block = chip + sign * k
            following = chip - sign

            @pl.when((block >= 0) & (block < n))
            def _(block=block, following=following, dev=dev):
                onward(block, c, dev, fs.at[block, c]).wait_recv()

                @pl.when((following >= 0) & (following < n))
                def _():
                    onward(block, c, dev, fs.at[block, c]).start()

                to_partner(block, c).start()

    def settle():
        for c in range(chunks):
            @pl.when(chip < n - 1)
            def _(c=c):
                onward(chip, c, right, own_s.at[0, c]).wait_send()

            @pl.when(chip > 0)
            def _(c=c):
                onward(chip, c, left, own_s.at[1, c]).wait_send()

            for d in range(n):
                to_partner((chip + d) % n, c).wait_send()
            for k in range(1, n):
                for sign, dev in ((-1, right), (1, left)):
                    block = chip + sign * k
                    following = chip - sign

                    @pl.when((block >= 0) & (block < n) & (following >= 0) & (following < n))
                    def _(block=block, dev=dev, c=c):
                        onward(block, c, dev, fs.at[block, c]).wait_send()

    tile = 256 if (3 * feats) % 256 == 0 else 128
    upper = chip // half
    near_side = chip * (1 - upper) + (n - 1 - chip) * upper
    far_sign = 1 - 2 * upper

    def block_at(t):
        if t == 0:
            return chip
        step = (t + 1) // 2
        two = step if t % 2 == 0 else -step
        past = (t - 1 - 2 * near_side + 2 * n) // (2 * n)
        return chip + two * (1 - past) + far_sign * (t - near_side) * past

    def own_copies(t, r):
        pieces = 4 if t == n - 1 else 1
        size = pair // pieces

        def copies(seg_from, seg_to, send, recv, to):
            return [
                remote(
                    kv_out.at[pl.ds(mul(seg_from * group + r + p * size, size), size), :],
                    kv_out.at[pl.ds(mul(seg_to * group + r + p * size, size), size), :],
                    send.at[t + p], recv.at[t + p], (to, s),
                )
                for p in range(pieces)
            ]

        return {
            "near01": copies(2, 1, a_s, a_r, 1),
            "far02": copies(2, 0, b_s, b_r, 2),
            "far13": copies(2, 0, b_s, b_r, 3),
            "near23": copies(2, 1, a_s, a_r, 3),
            "near32": copies(0, 1, a_s, a_r, 2),
        }

    own_sends = (("near01", "far02"), ("far13",), ("near23",), ("near32",))
    arrivals = ((), ("near01",), ("near32", "far02"), ("near23",))

    plan = []
    forwarded = []

    def forward_to(count):
        for t in range(len(forwarded), count):
            forwarded.append(t)

            @pl.when(m == 3)
            def _(t=t):
                for came, goes in zip(plan[t]["far13"], plan[t]["near32"]):
                    came.wait_recv()
                    goes.start()

    def project():
        t = len(plan)
        block = block_at(t)
        r = mul(block * pair, pair)
        mode = modality[m * n + block]
        for c in range(chunks):
            from_partner(block, c).wait_recv()

        def one_tile(j, carry):
            cols = pl.ds(mul(j * tile, tile), tile)
            stage[:, cols] = jnp.dot(
                xg[pl.ds(r, pair), :], wv[mode, :, cols], preferred_element_type=F32
            ).astype(BF16)
            return carry

        lax.fori_loop(0, 3 * feats // tile, one_tile, 0)
        for h in range(heads):
            q_out[pl.ds(r, pair), pl.ds(h * HDIM, HDIM)] = stage[:, pl.ds(3 * h * HDIM, HDIM)]
            kv_out[pl.ds(mul(2 * group + r, pair), pair), pl.ds(2 * h * HDIM, 2 * HDIM)] = stage[
                :, pl.ds((3 * h + 1) * HDIM, 2 * HDIM)
            ]
        copies = own_copies(t, r)
        plan.append(copies)
        for who in range(3):
            @pl.when(m == who)
            def _(who=who):
                for name in own_sends[who]:
                    for c in copies[name]:
                        c.start()
        forward_to(t)

    for c in range(chunks - 1):
        handle(1, c)
    for c in w_copies:
        c.wait()
    project()
    handle(1, chunks - 1)
    project()
    for k in range(2, n):
        for c in range(chunks):
            handle(k, c)
        project()
    squares = width // feats
    o_copies = [
        pltpu.make_async_copy(
            o_hbm.at[k, :, pl.ds(c * feats, feats)],
            wv.at[k, pl.ds(c * feats, feats), pl.ds(0, feats)],
            o_sem.at[k * squares + c],
        )
        for c in range(squares) for k in range(mods)
    ]
    for c in o_copies:
        c.start()
    forward_to(n)
    settle()
    for who in range(4):
        @pl.when(m == who)
        def _(who=who):
            for copies in plan:
                for name in arrivals[who]:
                    for c in copies[name]:
                        c.wait_recv()

    q, kv = q_out, kv_out
    keys = 3 * group
    chunk = keys
    while chunk > 1536:
        chunk //= 2
    scale = math.log2(math.e) / math.sqrt(HDIM)
    first_key = (m - 2) * group
    def mine(t):
        return pl.ds(mul(t * pair + core * rows, rows), rows)

    def theirs(t):
        return pl.ds(mul(t * pair + (1 - core) * rows, rows), rows)

    waited = []

    def compute(t, off):
        r = mul(((chip + off + n) % n) * pair, pair)
        pos = m * group + r + lax.broadcasted_iota(jnp.int32, (pair, 1), 0)
        end = jnp.int32(0)
        start = jnp.zeros((pair, 1), jnp.int32)
        for d in range(doc_lengths.shape[0]):
            end = end + doc_lengths[d]
            start = jnp.where(pos >= end, end, start)
        for c0 in range(0, keys, chunk):
            key = first_key + c0 + lax.broadcasted_iota(jnp.int32, (pair, chunk), 1)
            bias[:, pl.ds(c0, chunk)] = jnp.where((key <= pos) & (key >= start), 0.0, -1e30)
        for h in range(heads):
            query = q[pl.ds(r, pair), pl.ds(h * HDIM, HDIM)]
            top = total = acc = None
            for c0 in reversed(range(0, keys, chunk)):
                k_part = kv[pl.ds(c0, chunk), pl.ds(2 * h * HDIM, HDIM)]
                v_part = kv[pl.ds(c0, chunk), pl.ds((2 * h + 1) * HDIM, HDIM)]
                scores = lax.dot_general(
                    query, k_part, (((1,), (1,)), ((), ())), preferred_element_type=F32
                ) * scale + bias[:, pl.ds(c0, chunk)]
                peak = jnp.max(scores, axis=1, keepdims=True)
                new_top = peak if top is None else jnp.maximum(top, peak)
                weights = jnp.exp2(scores - new_top)
                if chunk != keys:
                    weights = jnp.where(bias[:, pl.ds(c0, chunk)] < 0.0, 0.0, weights)
                row_sum = jnp.sum(weights, axis=1, keepdims=True)
                added = jnp.dot(weights.astype(BF16), v_part, preferred_element_type=F32)
                if top is None:
                    total, acc = row_sum, added
                else:
                    fix = jnp.exp2(top - new_top)
                    total, acc = total * fix + row_sum, acc * fix + added
                top = new_top
            att[:, pl.ds(h * HDIM, HDIM)] = (acc / total).astype(BF16)
        if not waited:
            for c in o_copies:
                c.wait()
            waited.append(True)
        mode = modality[m * n + (chip + off + n) % n]

        def one_tile(j, carry):
            cols = pl.ds(mul(j * feats, feats), feats)
            square = wv[mode, cols, pl.ds(0, feats)]
            xg[pl.ds(t * pair, pair), cols] = jnp.dot(
                att[...], square, preferred_element_type=F32
            ).astype(BF16)
            return carry

        lax.fori_loop(0, squares, one_tile, 0)
        copy = remote(xg.at[theirs(t), :], pairbuf.at[t], ps2.at[t], pr2.at[t], partner)
        copy.start()
        return copy

    lo, hi = pl.ds(0, width // 2), pl.ds(width // 2, width // 2)
    sent = []

    def pair_sum(t, copy):
        copy.wait_recv()
        sent.append(copy)
        return xg[mine(t), :].astype(F32) + pairbuf[t].astype(F32)

    def send(src, dst, ss, rsm, dev):
        copy = remote(src, dst, ss, rsm, dev)
        copy.start()
        sent.append(copy)
        return copy

    copy = compute(0, half)
    xg[mine(0), :] = pair_sum(0, copy).astype(BF16)
    r_prev = send(xg.at[mine(0), lo], right_in.at[half - 1, :, lo], rs.at[half - 1], rr.at[half - 1], right)
    l_prev = send(xg.at[mine(0), hi], left_in.at[half - 1, :, hi], ls.at[half - 1], lr.at[half - 1], left)
    t = 1
    for k in range(half - 1, 0, -1):
        c_right = compute(t, k)
        c_left = compute(t + 1, -k)
        for which, (tt, c, prev, inbox, ss, rsm, dev, cols) in enumerate((
            (t, c_right, r_prev, right_in, rs, rr, right, lo),
            (t + 1, c_left, l_prev, left_in, ls, lr, left, hi),
        )):
            total = pair_sum(tt, c)
            prev.wait_recv()
            if k == half - 1:
                a, b = total[:, : width // 2], total[:, width // 2:]
                if which == 0:
                    a = a + inbox[k, :, lo].astype(F32)
                else:
                    b = b + inbox[k, :, hi].astype(F32)
                xg[mine(tt), lo] = a.astype(BF16)
                xg[mine(tt), hi] = b.astype(BF16)
            else:
                xg[mine(tt), :] = (total + inbox[k].astype(F32)).astype(BF16)
            new = send(xg.at[mine(tt), :], inbox.at[k - 1], ss.at[k - 1], rsm.at[k - 1], dev)
            if which == 0:
                r_prev = new
            else:
                l_prev = new
        t += 2
    c = compute(t, 0)
    total = pair_sum(t, c) + tokens[...].astype(F32)
    r_prev.wait_recv()
    total = total + right_in[0].astype(F32)
    l_prev.wait_recv()
    out[...] = (total + left_in[0].astype(F32)).astype(BF16)
    for copy in sent:
        copy.wait_send()


    for who in range(4):
        @pl.when(m == who)
        def _(who=who):
            for copies in plan:
                for name in own_sends[who]:
                    for c in copies[name]:
                        c.wait_send()


def body(n, tokens, norm_gain, qkv_weight, out_weight, modality, doc_lengths):
    rows, width = tokens.shape
    feats = out_weight.shape[1]
    mods = out_weight.shape[0]
    pair = 2 * rows
    group = n * pair
    half = n // 2
    vmem = pl.BlockSpec(memory_space=pltpu.VMEM)
    smem = pl.BlockSpec(memory_space=pltpu.SMEM)
    hbm = pl.BlockSpec(memory_space=pl.ANY)
    dma = pltpu.SemaphoreType.DMA
    limit = 62 * 1024 * 1024
    return pl.pallas_call(
        functools.partial(sublayer, n),
        out_shape=jax.ShapeDtypeStruct((rows, width), BF16),
        in_specs=[smem, smem, vmem, vmem, hbm, hbm],
        out_specs=vmem,
        scratch_shapes=[
            pltpu.VMEM((mods, width, 3 * feats), BF16),
            pltpu.VMEM((group, width), BF16),
            pltpu.VMEM((pair, 3 * feats), BF16),
            pltpu.VMEM((group, feats), BF16),
            pltpu.VMEM((3 * group, 2 * feats), BF16),
            pltpu.VMEM((pair, feats), BF16),
            pltpu.VMEM((n, rows, width), BF16),
            pltpu.VMEM((pair, 3 * group), F32),
            pltpu.VMEM((half, rows, width), BF16),
            pltpu.VMEM((half, rows, width), BF16),
            dma((mods,)), dma((mods * (width // feats),)),
            dma((2, 2)), dma((n, 2)), dma((n, 2)), dma((n, 2)), dma((n, 2)),
            dma((n + 3,)), dma((n + 3,)), dma((n + 3,)), dma((n + 3,)),
            dma((n,)), dma((n,)),
            dma((half,)), dma((half,)), dma((half,)), dma((half,)),
        ],
        compiler_params=pltpu.CompilerParams(
            collective_id=0, has_side_effects=True, vmem_limit_bytes=limit
        ),
    )(modality, doc_lengths, tokens, norm_gain, qkv_weight, out_weight)


def solution(mesh):
    return jax.shard_map(
        functools.partial(body, mesh.shape["seq"] // 2),
        mesh=mesh,
        in_specs=(
            P(("mod", "seq"), None),
            P(),
            P(None, None, "seq"),
            P(None, "seq", None),
            P(),
            P(),
        ),
        out_specs=P(("mod", "seq"), None),
        check_vma=False,
    )
```
